128 devices in a mesh: dap: 16 (over z, y), dp: 8 (over x, core).
Axes of the slice: x: 4, y: 4, z: 4, core: 2. Of those that a mesh axis runs over, the one named last changes fastest.
Arguments:
- pair_z: bfloat16 [32, 128, 128, 128], P('dp', 'dap')
- single_s: bfloat16 [32, 128, 384], P('dp', 'dap')
- token_mask: int32 [32, 128], P('dp')
- dz_out: bfloat16 [32, 128, 128, 128], P('dp', 'dap')
- ds_out: bfloat16 [32, 128, 384], P('dp', 'dap')
- w_pa: bfloat16 [128, 512], replicated
- w_pb: bfloat16 [128, 512], replicated
- w_po: bfloat16 [512, 128], replicated
- w_bias: bfloat16 [128, 16], replicated
- w_q: bfloat16 [384, 384], replicated
- q_bias: bfloat16 [384], replicated
- w_kv: bfloat16 [384, 768], replicated
- w_g: bfloat16 [384, 384], replicated
- w_o: bfloat16 [384, 384], replicated
- w_sa: bfloat16 [384, 1536], replicated
- w_sb: bfloat16 [384, 1536], replicated
- w_so: bfloat16 [1536, 384], replicated
Outputs:
- output 1: bfloat16 [32, 128, 128, 128], P('dp', 'dap')
- output 2: bfloat16 [32, 128, 384], P('dp', 'dap')
- output 3: float32 [128, 512], replicated
- output 4: float32 [128, 512], replicated
- output 5: float32 [512, 128], replicated
- output 6: float32 [128, 16], replicated
- output 7: float32 [384, 384], replicated
- output 8: float32 [384], replicated
- output 9: float32 [384, 768], replicated
- output 10: float32 [384, 384], replicated
- output 11: float32 [384, 384], replicated
- output 12: float32 [384, 1536], replicated
- output 13: float32 [384, 1536], replicated
- output 14: float32 [1536, 384], replicated
All inputs are finite; a program needn't handle non-finite values.
Results may differ from the reference program's by a relative error of at most 0.02.
Values are sent between devices in bfloat16 or wider.
A program may use at most 1 GiB of HBM per device.

```python
import jax
import jax.numpy as jnp
from jax import lax

C_S = 384
C_Z = 128
HEADS = 16
HEAD = 24
TRANS = 4
TOKENS = 128
COMPLEXES = 32


def snap_bf16(values):
    return values + lax.stop_gradient(values.astype(jnp.bfloat16).astype(jnp.float32) - values)


def layer_norm(values):
    centred = values - jnp.mean(values, axis=-1, keepdims=True)
    return centred * lax.rsqrt(jnp.mean(centred * centred, axis=-1, keepdims=True) + 1e-5)


def pair_rows(z_rows, w_pa, w_pb, w_po):
    normed = snap_bf16(layer_norm(z_rows))
    hid_a = jnp.einsum('rjc,cf->rjf', normed, w_pa)
    hid_b = jnp.einsum('rjc,cf->rjf', normed, w_pb)
    hidden = snap_bf16(jax.nn.silu(hid_a) * hid_b)
    return snap_bf16(z_rows + jnp.einsum('rjf,fc->rjc', hidden, w_po))


def block_forward(pair_z, single_s, mask_row, w_pa, w_pb, w_po, w_bias, w_q, q_bias, w_kv, w_g, w_o, w_sa, w_sb, w_so):
    attn_width = HEADS * HEAD
    checked_rows = jax.checkpoint(pair_rows)

    def row_step(z_rows):
        return checked_rows(z_rows, w_pa, w_pb, w_po)

    z_new = lax.map(row_step, pair_z.reshape(TOKENS // 16, 16, TOKENS, C_Z)).reshape(TOKENS, TOKENS, C_Z)
    pair_bias = jnp.einsum('ijc,ch->hij', snap_bf16(layer_norm(z_new)), w_bias)
    act_norm = snap_bf16(layer_norm(single_s))
    queries = snap_bf16(jnp.dot(act_norm, w_q, preferred_element_type=jnp.float32) + q_bias).reshape(TOKENS, HEADS, HEAD)
    key_val = snap_bf16(jnp.dot(act_norm, w_kv, preferred_element_type=jnp.float32))
    key_heads = key_val[:, :attn_width].reshape(TOKENS, HEADS, HEAD)
    value_heads = key_val[:, attn_width:].reshape(TOKENS, HEADS, HEAD)
    gate_vals = jax.nn.sigmoid(jnp.dot(act_norm, w_g, preferred_element_type=jnp.float32))
    key_mask = 1e9 * (mask_row.astype(jnp.float32) - 1.0)
    logits = jnp.einsum('ihd,jhd->hij', queries, key_heads) * (HEAD ** -0.5) + pair_bias + key_mask[None, None, :]
    attn_prob = snap_bf16(jax.nn.softmax(logits, axis=-1))
    attended = jnp.einsum('hij,jhd->ihd', attn_prob, value_heads).reshape(TOKENS, attn_width)
    gated = snap_bf16(gate_vals * attended)
    s_mid = snap_bf16(single_s + jnp.dot(gated, w_o, preferred_element_type=jnp.float32))
    mid_act = snap_bf16(layer_norm(s_mid))
    trans_a = jnp.dot(mid_act, w_sa, preferred_element_type=jnp.float32)
    trans_b = jnp.dot(mid_act, w_sb, preferred_element_type=jnp.float32)
    trans_hidden = snap_bf16(jax.nn.silu(trans_a) * trans_b)
    return z_new, s_mid + jnp.dot(trans_hidden, w_so, preferred_element_type=jnp.float32)


def draw_mask(mask_key):
    len_key, full_key = jax.random.split(mask_key)
    lengths = jax.random.randint(len_key, (COMPLEXES,), TOKENS // 4, TOKENS + 1)
    full_at = jax.random.randint(full_key, (), 0, COMPLEXES)
    lengths = jnp.where(jnp.arange(COMPLEXES) == full_at, TOKENS, lengths)
    return (jnp.arange(TOKENS)[None, :] < lengths[:, None]).astype(jnp.int32)


def setup_inputs(seed: int = 0) -> dict:
    sub_keys = jax.random.split(jax.random.key(seed), 17)
    attn_width = HEADS * HEAD

    def draw_normal(key_index, arr_shape, std_scale):
        return (jax.random.normal(sub_keys[key_index], arr_shape, jnp.float32) * std_scale).astype(jnp.bfloat16)

    return {
        'pair_z': draw_normal(0, (COMPLEXES, TOKENS, TOKENS, C_Z), 1.0),
        'single_s': draw_normal(1, (COMPLEXES, TOKENS, C_S), 1.0),
        'token_mask': draw_mask(sub_keys[2]),
        'dz_out': draw_normal(3, (COMPLEXES, TOKENS, TOKENS, C_Z), 1.0),
        'ds_out': draw_normal(4, (COMPLEXES, TOKENS, C_S), 1.0),
        'w_pa': draw_normal(5, (C_Z, TRANS * C_Z), C_Z ** -0.5),
        'w_pb': draw_normal(6, (C_Z, TRANS * C_Z), C_Z ** -0.5),
        'w_po': draw_normal(7, (TRANS * C_Z, C_Z), (TRANS * C_Z) ** -0.5),
        'w_bias': draw_normal(8, (C_Z, HEADS), C_Z ** -0.5),
        'w_q': draw_normal(9, (C_S, attn_width), C_S ** -0.5),
        'q_bias': draw_normal(10, (attn_width,), 0.5),
        'w_kv': draw_normal(11, (C_S, 2 * attn_width), C_S ** -0.5),
        'w_g': draw_normal(12, (C_S, attn_width), C_S ** -0.5),
        'w_o': draw_normal(13, (attn_width, C_S), attn_width ** -0.5),
        'w_sa': draw_normal(14, (C_S, TRANS * C_S), C_S ** -0.5),
        'w_sb': draw_normal(15, (C_S, TRANS * C_S), C_S ** -0.5),
        'w_so': draw_normal(16, (TRANS * C_S, C_S), (TRANS * C_S) ** -0.5),
    }


def reference(pair_z, single_s, token_mask, dz_out, ds_out, w_pa, w_pb, w_po, w_bias, w_q, q_bias, w_kv, w_g, w_o, w_sa, w_sb, w_so):
    weights = tuple(weight.astype(jnp.float32) for weight in (w_pa, w_pb, w_po, w_bias, w_q, q_bias, w_kv, w_g, w_o, w_sa, w_sb, w_so))

    def scan_step(running, per_complex):
        z_one, s_one, mask_one, dz_one, ds_one = per_complex

        def run_block(z_in, s_in, *params):
            return block_forward(z_in, s_in, mask_one, *params)

        _, pullback = jax.vjp(run_block, z_one.astype(jnp.float32), s_one.astype(jnp.float32), *weights)
        all_grads = pullback((dz_one.astype(jnp.float32), ds_one.astype(jnp.float32)))
        summed = tuple(acc_sum + update for acc_sum, update in zip(running, all_grads[2:]))
        return summed, (all_grads[0].astype(jnp.bfloat16), all_grads[1].astype(jnp.bfloat16))

    zero_sums = tuple(jnp.zeros_like(weight) for weight in weights)
    grad_sums, (dz_in, ds_in) = lax.scan(scan_step, zero_sums, (pair_z, single_s, token_mask, dz_out, ds_out))
    return (dz_in, ds_in, grad_sums[0], grad_sums[1], grad_sums[2], grad_sums[3], grad_sums[4], grad_sums[5], grad_sums[6], grad_sums[7], grad_sums[8], grad_sums[9], grad_sums[10], grad_sums[11])
```

```python
import functools

import jax
import jax.numpy as jnp
from jax import lax
from jax.experimental import pallas as pl
from jax.experimental.pallas import tpu as pltpu
from jax.sharding import PartitionSpec as P

HEAD_DIM = 24
EPSILON = 1e-5
MASK_BIG = 1e9
BLOCK = 512
F32 = jnp.float32
BF16 = jnp.bfloat16


def mm(lhs, rhs):
    return lax.dot_general(lhs, rhs, (((1,), (0,)), ((), ())), preferred_element_type=F32)


def mm_nt(lhs, rhs):
    return lax.dot_general(lhs, rhs, (((1,), (1,)), ((), ())), preferred_element_type=F32)


def mm_tn(lhs, rhs):
    return lax.dot_general(lhs, rhs, (((0,), (0,)), ((), ())), preferred_element_type=F32)


def layer_norm(values):
    wide_vals = values.astype(F32)
    centred = wide_vals - jnp.mean(wide_vals, axis=-1, keepdims=True)
    inv_std = lax.rsqrt(jnp.mean(centred * centred, axis=-1, keepdims=True) + EPSILON)
    return centred * inv_std, inv_std


def norm_grad(normed, inv_std, grad_out):
    mean_grad = jnp.mean(grad_out, axis=-1, keepdims=True)
    mean_proj = jnp.mean(grad_out * normed, axis=-1, keepdims=True)
    return inv_std * (grad_out - mean_grad - normed * mean_proj)


def sigmoid(values):
    return 0.5 + 0.5 * jnp.tanh(0.5 * values)


def swiglu(hid_a, hid_b):
    half = 0.5 * hid_a
    return half * (1.0 + jnp.tanh(half)) * hid_b


def swiglu_and_grad(hid_a, hid_b, grad_hidden):
    half = 0.5 * hid_a
    plus = 1.0 + jnp.tanh(half)
    silu = half * plus
    sig = 0.5 * plus
    grad_b = grad_hidden * silu
    grad_a = grad_hidden * hid_b * (sig + silu * (1.0 - sig))
    return silu * hid_b, grad_a, grad_b


def pair_forward_kernel(z_ref, w_ab_ref, w_po_ref, w_bias_t_ref, z_new_ref, bias_ref):
    width = w_po_ref.shape[0]
    z_rows = z_ref[...]
    normed, _ = layer_norm(z_rows)
    hid = mm(normed.astype(BF16), w_ab_ref[...])
    hidden = swiglu(hid[:, :width], hid[:, width:]).astype(BF16)
    z_new = (z_rows.astype(F32) + mm(hidden, w_po_ref[...])).astype(BF16)
    z_new_ref[...] = z_new
    bias_norm, _ = layer_norm(z_new)
    bias = mm_nt(w_bias_t_ref[...], bias_norm.astype(BF16))
    heads = w_bias_t_ref.shape[0]
    tok = bias_ref.shape[1]
    for row in range(bias.shape[1] // tok):
        bias_ref[row * heads:(row + 1) * heads, :] = bias[:, row * tok:(row + 1) * tok]


def pair_forward(z_rows, w_ab, w_po, w_bias_t, tok):
    rows, chan = z_rows.shape
    heads = w_bias_t.shape[0]
    width = w_po.shape[0]
    whole = lambda shape: pl.BlockSpec(shape, lambda i: (0, 0))
    return pl.pallas_call(
        pair_forward_kernel,
        grid=(rows // BLOCK,),
        in_specs=[pl.BlockSpec((BLOCK, chan), lambda i: (i, 0)), whole((chan, 2 * width)), whole((width, chan)), whole((heads, chan))],
        out_specs=[pl.BlockSpec((BLOCK, chan), lambda i: (i, 0)), pl.BlockSpec((BLOCK // tok * heads, tok), lambda i: (i, 0))],
        out_shape=[jax.ShapeDtypeStruct((rows, chan), BF16), jax.ShapeDtypeStruct((rows // tok * heads, tok), F32)],
        name="pair_forward",
        cost_estimate=pl.CostEstimate(flops=6 * rows * chan * width, bytes_accessed=4 * rows * chan, transcendentals=0),
    )(z_rows, w_ab, w_po, w_bias_t)


def pair_backward_kernel(z_ref, zn_ref, dz_ref, gl_ref, w_ab_ref, w_ab_t_ref, w_po_t_ref, w_bias_t_ref, dzi_ref, dwab_ref, dwpo_t_ref, dwb_t_ref):
    width = w_po_t_ref.shape[1]
    heads = w_bias_t_ref.shape[0]

    @pl.when(pl.program_id(0) == 0)
    def _():
        dwab_ref[...] = jnp.zeros_like(dwab_ref)
        dwpo_t_ref[...] = jnp.zeros_like(dwpo_t_ref)
        dwb_t_ref[...] = jnp.zeros_like(dwb_t_ref)

    bias_norm, bias_inv = layer_norm(zn_ref[...])
    groups = gl_ref.shape[0] // heads
    gl = jnp.concatenate([gl_ref[k * heads:(k + 1) * heads, :] for k in range(groups)], axis=1)
    dwb_t_ref[...] += mm(gl, bias_norm.astype(BF16))
    grad_norm = mm_tn(gl, w_bias_t_ref[...])
    grad_new = dz_ref[...].astype(F32) + norm_grad(bias_norm, bias_inv, grad_norm)
    grad_new_bf = grad_new.astype(BF16)
    normed, inv_std = layer_norm(z_ref[...])
    normed_bf = normed.astype(BF16)
    hid = mm(normed_bf, w_ab_ref[...])
    grad_hidden = mm(grad_new_bf, w_po_t_ref[...])
    hidden, grad_a, grad_b = swiglu_and_grad(hid[:, :width], hid[:, width:], grad_hidden)
    dwpo_t_ref[...] += mm_tn(grad_new_bf, hidden.astype(BF16))
    grad_ab = jnp.concatenate([grad_a.astype(BF16), grad_b.astype(BF16)], axis=1)
    dwab_ref[...] += mm_tn(normed_bf, grad_ab)
    grad_normed = mm(grad_ab, w_ab_t_ref[...])
    dzi_ref[...] = (grad_new + norm_grad(normed, inv_std, grad_normed)).astype(BF16)


def pair_backward(z_rows, z_new, dz_rows, grad_logits, w_ab, w_ab_t, w_po_t, w_bias_t, tok):
    rows, chan = z_rows.shape
    heads = w_bias_t.shape[0]
    width = w_po_t.shape[1]
    whole = lambda shape: pl.BlockSpec(shape, lambda i: (0, 0))
    row_spec = pl.BlockSpec((BLOCK, chan), lambda i: (i, 0))
    return pl.pallas_call(
        pair_backward_kernel,
        grid=(rows // BLOCK,),
        in_specs=[row_spec, row_spec, row_spec, pl.BlockSpec((BLOCK // tok * heads, tok), lambda i: (i, 0)), whole((chan, 2 * width)), whole((2 * width, chan)), whole((chan, width)), whole((heads, chan))],
        out_specs=[row_spec, whole((chan, 2 * width)), whole((chan, width)), whole((heads, chan))],
        out_shape=[jax.ShapeDtypeStruct((rows, chan), BF16), jax.ShapeDtypeStruct((chan, 2 * width), F32), jax.ShapeDtypeStruct((chan, width), F32), jax.ShapeDtypeStruct((heads, chan), F32)],
        name="pair_backward",
        cost_estimate=pl.CostEstimate(flops=16 * rows * chan * width, bytes_accessed=8 * rows * chan, transcendentals=0),
    )(z_rows, z_new, dz_rows, grad_logits, w_ab, w_ab_t, w_po_t, w_bias_t)


def single_kernel(tok, s_all_ref, s_ref, ds_ref, mask_ref, bias_ref, w_q_ref, q_bias_ref, w_kv_ref, w_g_ref, w_o_ref, w_sa_ref, w_sb_ref, w_so_ref,
                  gl_ref, part_ref, gact_ref, gmid_ref, dwq_ref, dqb_ref, dwkv_ref, dwg_ref, dwo_ref, dwsa_ref, dwsb_ref, dwso_ref,
                  q_exp, g_exp, prob, gkv):
    rows, chan = s_ref.shape
    num_cplx = s_all_ref.shape[0] // tok
    heads = bias_ref.shape[0] // rows
    per = rows // num_cplx * heads
    scale = HEAD_DIM ** -0.5
    flat = rows * heads

    def expand(values):
        pick = lax.broadcasted_iota(jnp.int32, (flat, rows), 0) // heads == lax.broadcasted_iota(jnp.int32, (flat, rows), 1)
        return mm(pick.astype(BF16), values)

    def head_mask(count):
        head = lax.broadcasted_iota(jnp.int32, (count, chan), 0) % heads
        col = lax.broadcasted_iota(jnp.int32, (count, chan), 1)
        return (col >= head * HEAD_DIM) & (col < head * HEAD_DIM + HEAD_DIM)

    def fold(values):
        kept = jnp.where(head_mask(values.shape[0]), values, 0.0)
        return jnp.sum(kept.reshape(values.shape[0] // heads, heads, chan), axis=1)

    a_all, _ = layer_norm(s_all_ref[...])
    a_all = a_all.astype(BF16)
    kv = mm(a_all, w_kv_ref[...]).astype(BF16)
    s_wide = s_ref[...].astype(F32)
    s_norm, _ = layer_norm(s_wide)
    act = s_norm.astype(BF16)
    queries = (mm(act, w_q_ref[...]) + q_bias_ref[...].astype(F32)).astype(BF16)
    gate = sigmoid(mm(act, w_g_ref[...]))
    q_exp[...] = jnp.where(head_mask(flat), expand(queries), 0.0).astype(BF16)
    key_mask = MASK_BIG * (mask_ref[...].astype(F32) - 1.0)
    attended = []
    for b in range(num_cplx):
        keys = kv[b * tok:(b + 1) * tok, :chan]
        vals = kv[b * tok:(b + 1) * tok, chan:]
        logits = mm_nt(q_exp[b * per:(b + 1) * per, :], keys) * scale + bias_ref[b * per:(b + 1) * per, :] + key_mask[b:b + 1, :]
        weight = jnp.exp(logits - jnp.max(logits, axis=-1, keepdims=True))
        p_wide = weight / jnp.sum(weight, axis=-1, keepdims=True)
        prob[b * per:(b + 1) * per, :] = p_wide
        attended.append(fold(mm(p_wide.astype(BF16), vals)))
    attended = jnp.concatenate(attended, axis=0)
    gated = (gate * attended).astype(BF16)
    s_mid = (s_wide + mm(gated, w_o_ref[...])).astype(BF16)
    mid_norm, mid_inv = layer_norm(s_mid)
    mid_act = mid_norm.astype(BF16)
    trans_a = mm(mid_act, w_sa_ref[...])
    trans_b = mm(mid_act, w_sb_ref[...])
    ds_rows = ds_ref[...]
    grad_hidden = mm_nt(ds_rows, w_so_ref[...])
    hidden, grad_ta, grad_tb = swiglu_and_grad(trans_a, trans_b, grad_hidden)
    grad_ta = grad_ta.astype(BF16)
    grad_tb = grad_tb.astype(BF16)
    dwso_ref[...] = mm_tn(hidden.astype(BF16), ds_rows)
    dwsa_ref[...] = mm_tn(mid_act, grad_ta)
    dwsb_ref[...] = mm_tn(mid_act, grad_tb)
    grad_mid_norm = mm_nt(grad_ta, w_sa_ref[...]) + mm_nt(grad_tb, w_sb_ref[...])
    grad_mid = ds_rows.astype(F32) + norm_grad(mid_norm, mid_inv, grad_mid_norm)
    grad_mid_bf = grad_mid.astype(BF16)
    gmid_ref[...] = grad_mid
    dwo_ref[...] = mm_tn(gated, grad_mid_bf)
    grad_gated = mm_nt(grad_mid_bf, w_o_ref[...])
    grad_gate = (grad_gated * attended * gate * (1.0 - gate)).astype(BF16)
    grad_att = (grad_gated * gate).astype(BF16)
    g_exp[...] = jnp.where(head_mask(flat), expand(grad_att), 0.0).astype(BF16)
    grad_query = []
    for b in range(num_cplx):
        keys = kv[b * tok:(b + 1) * tok, :chan]
        vals = kv[b * tok:(b + 1) * tok, chan:]
        p_wide = prob[b * per:(b + 1) * per, :]
        g_rows = g_exp[b * per:(b + 1) * per, :]
        grad_prob = mm_nt(g_rows, vals)
        grad_logits = (p_wide * (grad_prob - jnp.sum(p_wide * grad_prob, axis=-1, keepdims=True))).astype(BF16)
        gl_ref[b * per:(b + 1) * per, :] = grad_logits
        grad_query.append(fold(mm(grad_logits, keys)) * scale)
        gkv[b * tok:(b + 1) * tok, :chan] = (mm_tn(grad_logits, q_exp[b * per:(b + 1) * per, :]) * scale).astype(BF16)
        gkv[b * tok:(b + 1) * tok, chan:] = mm_tn(p_wide.astype(BF16), g_rows).astype(BF16)
    grad_query = jnp.concatenate(grad_query, axis=0)
    grad_query_bf = grad_query.astype(BF16)
    dwkv_ref[...] = mm_tn(a_all, gkv[...])
    part_ref[...] = mm_nt(gkv[...], w_kv_ref[...]).astype(BF16)
    dwq_ref[...] = mm_tn(act, grad_query_bf)
    dqb_ref[...] = jnp.sum(grad_query, axis=0, keepdims=True)
    dwg_ref[...] = mm_tn(act, grad_gate)
    gact_ref[...] = mm_nt(grad_query_bf, w_q_ref[...]) + mm_nt(grad_gate, w_g_ref[...])


def single_track(tok, s_all, s_rows, ds_rows, mask, bias, weights):
    rows, chan = s_rows.shape
    flat = bias.shape[0]
    all_rows = s_all.shape[0]
    shapes = [((flat, tok), BF16), ((all_rows, chan), BF16), ((rows, chan), F32), ((rows, chan), F32)] + [(w.shape, F32) for w in weights]
    return pl.pallas_call(
        functools.partial(single_kernel, tok),
        out_shape=[jax.ShapeDtypeStruct(*s) for s in shapes],
        in_specs=[pl.BlockSpec(memory_space=pltpu.VMEM)] * (5 + len(weights)),
        out_specs=[pl.BlockSpec(memory_space=pltpu.VMEM)] * len(shapes),
        scratch_shapes=[pltpu.VMEM((flat, chan), BF16), pltpu.VMEM((flat, chan), BF16), pltpu.VMEM((flat, tok), F32), pltpu.VMEM((all_rows, 2 * chan), BF16)],
        name="single_track",
        cost_estimate=pl.CostEstimate(flops=3 * 10**9, bytes_accessed=20 * 2**20, transcendentals=0),
    )(s_all, s_rows, ds_rows, mask, bias, *weights)


def solution(mesh):
    pair_spec = P('dp', 'dap', None, None)
    single_spec = P('dp', 'dap', None)

    def body(pair_z, single_s, token_mask, dz_out, ds_out, w_pa, w_pb, w_po, w_bias, w_q, q_bias, w_kv, w_g, w_o, w_sa, w_sb, w_so):
        num_cplx, num_rows, tok, pair_dim = pair_z.shape
        chan = single_s.shape[-1]
        width = w_pa.shape[1]
        w_ab = jnp.concatenate([w_pa, w_pb], axis=1)
        w_ab_t = w_ab.T
        w_bias_t = w_bias.T
        z_rows = pair_z.reshape(-1, pair_dim)
        dz_rows = dz_out.reshape(-1, pair_dim)
        s_all = lax.all_gather(single_s, 'dap', axis=1, tiled=True).reshape(-1, chan)
        z_new, bias = pair_forward(z_rows, w_ab, w_po, w_bias_t, tok)
        s_rows = single_s.reshape(-1, chan)
        outs = single_track(tok, s_all, s_rows, ds_out.reshape(-1, chan), token_mask, bias, (w_q, q_bias[None], w_kv, w_g, w_o, w_sa, w_sb, w_so))
        grad_logits, part, gact, gmid = outs[:4]
        dwq, dqb, dwkv, dwg, dwo, dwsa, dwsb, dwso = outs[4:]
        part_sum = lax.psum_scatter(part.reshape(num_cplx, -1, chan), 'dap', scatter_dimension=1, tiled=True)
        s_norm, s_inv = layer_norm(s_rows)
        ds_in = (gmid + norm_grad(s_norm, s_inv, gact + part_sum.reshape(-1, chan).astype(F32))).astype(BF16)
        dz_in, dwab, dwpo_t, dwb_t = pair_backward(z_rows, z_new, dz_rows, grad_logits, w_ab, w_ab_t, w_po.T, w_bias_t, tok)
        grads = (dwab[:, :width], dwab[:, width:], dwpo_t.T, dwb_t.T, dwq, dqb[0], dwkv, dwg, dwo, dwsa, dwsb, dwso)
        grads = lax.psum(grads, ('dap', 'dp'))
        return (dz_in.reshape(pair_z.shape), ds_in.reshape(single_s.shape)) + tuple(grads)

    in_specs = (pair_spec, single_spec, P('dp', None), pair_spec, single_spec) + (P(),) * 12
    out_specs = (pair_spec, single_spec) + (P(),) * 12
    return jax.shard_map(body, mesh=mesh, in_specs=in_specs, out_specs=out_specs, check_vma=False)
```

```python
import functools

import jax
import jax.numpy as jnp
from jax import lax
from jax.experimental import pallas as pl
from jax.experimental.pallas import tpu as pltpu
from jax.sharding import PartitionSpec as P

HEAD_DIM = 24
EPSILON = 1e-5
MASK_BIG = 1e9
BLOCK = 512
SIDE = 4
PLANE = 16
LANES = 128
SHARDS = 96
PIECE_ROWS = (144, 64, 16)
ROUTES = (('x', 'y', 'z'), ('y', 'z', 'x'), ('z', 'x', 'y'))
MESH = pl.DeviceIdType.MESH
F32 = jnp.float32
BF16 = jnp.bfloat16


def mm(lhs, rhs):
    return lax.dot_general(lhs, rhs, (((1,), (0,)), ((), ())), preferred_element_type=F32)


def mm_nt(lhs, rhs):
    return lax.dot_general(lhs, rhs, (((1,), (1,)), ((), ())), preferred_element_type=F32)


def mm_tn(lhs, rhs):
    return lax.dot_general(lhs, rhs, (((0,), (0,)), ((), ())), preferred_element_type=F32)


def layer_norm(values):
    wide_vals = values.astype(F32)
    centred = wide_vals - jnp.mean(wide_vals, axis=-1, keepdims=True)
    inv_std = lax.rsqrt(jnp.mean(centred * centred, axis=-1, keepdims=True) + EPSILON)
    return centred * inv_std, inv_std


def norm_grad(normed, inv_std, grad_out):
    mean_grad = jnp.mean(grad_out, axis=-1, keepdims=True)
    mean_proj = jnp.mean(grad_out * normed, axis=-1, keepdims=True)
    return inv_std * (grad_out - mean_grad - normed * mean_proj)


def sigmoid(values):
    return 0.5 + 0.5 * jnp.tanh(0.5 * values)


def swiglu(hid_a, hid_b):
    half = 0.5 * hid_a
    return half * (1.0 + jnp.tanh(half)) * hid_b


def swiglu_and_grad(hid_a, hid_b, grad_hidden):
    half = 0.5 * hid_a
    plus = 1.0 + jnp.tanh(half)
    silu = half * plus
    sig = 0.5 * plus
    grad_b = grad_hidden * silu
    grad_a = grad_hidden * hid_b * (sig + silu * (1.0 - sig))
    return silu * hid_b, grad_a, grad_b


def position():
    dap = lax.axis_index('dap')
    dp = lax.axis_index('dp')
    return {'dap': dap, 'dp': dp, 'z': dap // SIDE, 'y': dap % SIDE, 'x': dp // 2, 'core': dp % 2}


def neighbour(here, axis, step):
    moved = (here[axis] + step) % SIDE
    if axis == 'x':
        return {'dap': here['dap'], 'dp': moved * 2 + here['core']}
    if axis == 'y':
        return {'dap': here['z'] * SIDE + moved, 'dp': here['dp']}
    return {'dap': moved * SIDE + here['y'], 'dp': here['dp']}


def plane_member(here, step):
    return {'dap': (here['dap'] + step) % PLANE, 'dp': here['dp']}


def partner(here):
    return {'dap': here['dap'], 'dp': here['x'] * 2 + 1 - here['core']}


def meet(devices):
    barrier = pltpu.get_barrier_semaphore()
    for device in devices:
        pl.semaphore_signal(barrier, inc=1, device_id=device, device_id_type=MESH)
    pl.semaphore_wait(barrier, len(devices))


def send(src, dst, send_sem, recv_sem, device):
    pltpu.make_async_remote_copy(src_ref=src, dst_ref=dst, send_sem=send_sem, recv_sem=recv_sem, device_id=device, device_id_type=MESH).start()


def wait_bytes(like, sem):
    pltpu.make_async_copy(like, like, sem).wait()


def pair_forward_kernel(z_ref, w_ab_ref, w_po_ref, w_bias_t_ref, s_ref, z_new_ref, bias_ref, bias_norm_ref, s_all_ref, held, send_sem, recv_sem):
    here = position()
    step = pl.program_id(0)

    @pl.when(step == 0)
    def _():
        meet([plane_member(here, k) for k in range(1, PLANE)])
        for k in range(1, PLANE):
            send(s_ref, held.at[here['dap']], send_sem, recv_sem, plane_member(here, k))
        held[here['dap']] = s_ref[...]

    width = w_po_ref.shape[0]
    z_rows = z_ref[...]
    normed, _ = layer_norm(z_rows)
    hid = mm(normed.astype(BF16), w_ab_ref[...])
    hidden = swiglu(hid[:, :width], hid[:, width:]).astype(BF16)
    z_new = (z_rows.astype(F32) + mm(hidden, w_po_ref[...])).astype(BF16)
    z_new_ref[...] = z_new
    bias_norm, _ = layer_norm(z_new)
    bias_norm = bias_norm.astype(BF16)
    bias_norm_ref[...] = bias_norm
    bias = mm_nt(w_bias_t_ref[...], bias_norm)
    heads = w_bias_t_ref.shape[0]
    tok = bias_ref.shape[1]
    for row in range(bias.shape[1] // tok):
        bias_ref[row * heads:(row + 1) * heads, :] = bias[:, row * tok:(row + 1) * tok]

    @pl.when(step == pl.num_programs(0) - 1)
    def _():
        others = held.at[pl.ds(0, PLANE - 1)]
        wait_bytes(others, recv_sem)
        wait_bytes(others, send_sem)
        s_all_ref[...] = held[...]


def pair_forward(z_rows, w_ab, w_po, w_bias_t, s_rows, tok):
    rows, chan = z_rows.shape
    heads = w_bias_t.shape[0]
    width = w_po.shape[0]
    whole = lambda shape: pl.BlockSpec(shape, lambda i: (0,) * len(shape))
    row_spec = pl.BlockSpec((BLOCK, chan), lambda i: (i, 0))
    return pl.pallas_call(
        pair_forward_kernel,
        grid=(rows // BLOCK,),
        in_specs=[row_spec, whole((chan, 2 * width)), whole((width, chan)), whole((heads, chan)), whole(s_rows.shape)],
        out_specs=[row_spec, pl.BlockSpec((BLOCK // tok * heads, tok), lambda i: (i, 0)), row_spec, whole((PLANE,) + s_rows.shape)],
        out_shape=[jax.ShapeDtypeStruct((rows, chan), BF16), jax.ShapeDtypeStruct((rows // tok * heads, tok), F32), jax.ShapeDtypeStruct((rows, chan), BF16), jax.ShapeDtypeStruct((PLANE,) + s_rows.shape, BF16)],
        scratch_shapes=[pltpu.VMEM((PLANE,) + s_rows.shape, BF16), pltpu.SemaphoreType.DMA, pltpu.SemaphoreType.DMA],
        compiler_params=pltpu.CompilerParams(collective_id=0, has_side_effects=True),
        name="pair_forward",
        cost_estimate=pl.CostEstimate(flops=6 * rows * chan * width, bytes_accessed=4 * rows * chan, transcendentals=0),
    )(z_rows, w_ab, w_po, w_bias_t, s_rows)


def pair_backward_kernel(z_ref, zn_ref, dz_ref, gl_ref, w_ab_ref, w_ab_t_ref, w_po_t_ref, w_bias_t_ref, dzi_ref, dwab_ref, dwpo_t_ref):
    width = w_po_t_ref.shape[1]
    heads = w_bias_t_ref.shape[0]

    @pl.when(pl.program_id(0) == 0)
    def _():
        dwab_ref[...] = jnp.zeros_like(dwab_ref)
        dwpo_t_ref[...] = jnp.zeros_like(dwpo_t_ref)

    bias_norm, bias_inv = layer_norm(zn_ref[...])
    groups = gl_ref.shape[0] // heads
    gl = jnp.concatenate([gl_ref[k * heads:(k + 1) * heads, :] for k in range(groups)], axis=1)
    grad_norm = mm_tn(gl, w_bias_t_ref[...])
    grad_new = dz_ref[...].astype(F32) + norm_grad(bias_norm, bias_inv, grad_norm)
    grad_new_bf = grad_new.astype(BF16)
    normed, inv_std = layer_norm(z_ref[...])
    normed_bf = normed.astype(BF16)
    hid = mm(normed_bf, w_ab_ref[...])
    grad_hidden = mm(grad_new_bf, w_po_t_ref[...])
    hidden, grad_a, grad_b = swiglu_and_grad(hid[:, :width], hid[:, width:], grad_hidden)
    dwpo_t_ref[...] += mm_tn(grad_new_bf, hidden.astype(BF16))
    grad_ab = jnp.concatenate([grad_a.astype(BF16), grad_b.astype(BF16)], axis=1)
    dwab_ref[...] += mm_tn(normed_bf, grad_ab)
    grad_normed = mm(grad_ab, w_ab_t_ref[...])
    dzi_ref[...] = (grad_new + norm_grad(normed, inv_std, grad_normed)).astype(BF16)


def pair_backward(z_rows, z_new, dz_rows, grad_logits, w_ab, w_ab_t, w_po_t, w_bias_t, tok):
    rows, chan = z_rows.shape
    heads = w_bias_t.shape[0]
    width = w_po_t.shape[1]
    whole = lambda shape: pl.BlockSpec(shape, lambda i: (0, 0))
    row_spec = pl.BlockSpec((BLOCK, chan), lambda i: (i, 0))
    return pl.pallas_call(
        pair_backward_kernel,
        grid=(rows // BLOCK,),
        in_specs=[row_spec, row_spec, row_spec, pl.BlockSpec((BLOCK // tok * heads, tok), lambda i: (i, 0)), whole((chan, 2 * width)), whole((2 * width, chan)), whole((chan, width)), whole((heads, chan))],
        out_specs=[row_spec, whole((chan, 2 * width)), whole((chan, width))],
        out_shape=[jax.ShapeDtypeStruct((rows, chan), BF16), jax.ShapeDtypeStruct((chan, 2 * width), F32), jax.ShapeDtypeStruct((chan, width), F32)],
        name="pair_backward",
        cost_estimate=pl.CostEstimate(flops=16 * rows * chan * width, bytes_accessed=8 * rows * chan, transcendentals=0),
    )(z_rows, z_new, dz_rows, grad_logits, w_ab, w_ab_t, w_po_t, w_bias_t)


def put(ref, offset, matrix):
    rows, cols = matrix.shape
    for j in range(cols // LANES):
        ref[offset + j * rows:offset + (j + 1) * rows, :] = matrix[:, j * LANES:(j + 1) * LANES].astype(BF16)
    return offset + cols // LANES * rows


def single_kernel(tok, s_all_ref, s_ref, ds_ref, mask_ref, bias_ref, bias_norm_ref, w_q_ref, q_bias_ref, w_kv_ref, w_g_ref, w_o_ref, w_sa_ref, w_sb_ref, w_so_ref,
                  gl_ref, part_ref, gact_ref, gmid_ref, wide_ref, attn_ref,
                  q_exp, g_exp, prob, gkv, stage):
    rows, chan = s_ref.shape
    num_cplx = s_all_ref.shape[0] * rows // tok
    row_count = rows // num_cplx
    heads = bias_ref.shape[0] // rows
    per = row_count * heads
    scale = HEAD_DIM ** -0.5
    flat = rows * heads

    def expand(values):
        pick = lax.broadcasted_iota(jnp.int32, (flat, rows), 0) // heads == lax.broadcasted_iota(jnp.int32, (flat, rows), 1)
        return mm(pick.astype(BF16), values)

    def head_mask(count):
        head = lax.broadcasted_iota(jnp.int32, (count, chan), 0) % heads
        col = lax.broadcasted_iota(jnp.int32, (count, chan), 1)
        return (col >= head * HEAD_DIM) & (col < head * HEAD_DIM + HEAD_DIM)

    def fold(values):
        kept = jnp.where(head_mask(values.shape[0]), values, 0.0)
        return jnp.sum(kept.reshape(values.shape[0] // heads, heads, chan), axis=1)

    a_wide, _ = layer_norm(s_all_ref[...])
    a_wide = jnp.concatenate([a_wide[:, b * row_count:(b + 1) * row_count, :].reshape(tok, chan) for b in range(num_cplx)], axis=0)
    a_all = a_wide.astype(BF16)
    kv = mm(a_all, w_kv_ref[...]).astype(BF16)
    s_wide = s_ref[...].astype(F32)
    s_norm, _ = layer_norm(s_wide)
    act = s_norm.astype(BF16)
    queries = (mm(act, w_q_ref[...]) + q_bias_ref[...].astype(F32)).astype(BF16)
    gate = sigmoid(mm(act, w_g_ref[...]))
    q_exp[...] = jnp.where(head_mask(flat), expand(queries), 0.0).astype(BF16)
    key_mask = MASK_BIG * (mask_ref[...].astype(F32) - 1.0)
    attended = []
    for b in range(num_cplx):
        keys = kv[b * tok:(b + 1) * tok, :chan]
        vals = kv[b * tok:(b + 1) * tok, chan:]
        logits = mm_nt(q_exp[b * per:(b + 1) * per, :], keys) * scale + bias_ref[b * per:(b + 1) * per, :] + key_mask[b:b + 1, :]
        weight = jnp.exp(logits - jnp.max(logits, axis=-1, keepdims=True))
        p_wide = weight / jnp.sum(weight, axis=-1, keepdims=True)
        prob[b * per:(b + 1) * per, :] = p_wide
        attended.append(fold(mm(p_wide.astype(BF16), vals)))
    attended = jnp.concatenate(attended, axis=0)
    gated = (gate * attended).astype(BF16)
    s_mid = (s_wide + mm(gated, w_o_ref[...])).astype(BF16)
    mid_norm, mid_inv = layer_norm(s_mid)
    mid_act = mid_norm.astype(BF16)
    trans_a = mm(mid_act, w_sa_ref[...])
    trans_b = mm(mid_act, w_sb_ref[...])
    ds_rows = ds_ref[...]
    grad_hidden = mm_nt(ds_rows, w_so_ref[...])
    hidden, grad_ta, grad_tb = swiglu_and_grad(trans_a, trans_b, grad_hidden)
    grad_ta = grad_ta.astype(BF16)
    grad_tb = grad_tb.astype(BF16)
    at = put(wide_ref, 0, mm_tn(mid_act, grad_ta))
    at = put(wide_ref, at, mm_tn(mid_act, grad_tb))
    put(wide_ref, at, mm_tn(hidden.astype(BF16), ds_rows))
    grad_mid_norm = mm_nt(grad_ta, w_sa_ref[...]) + mm_nt(grad_tb, w_sb_ref[...])
    grad_mid = ds_rows.astype(F32) + norm_grad(mid_norm, mid_inv, grad_mid_norm)
    grad_mid_bf = grad_mid.astype(BF16)
    gmid_ref[...] = grad_mid
    grad_gated = mm_nt(grad_mid_bf, w_o_ref[...])
    grad_gate = (grad_gated * attended * gate * (1.0 - gate)).astype(BF16)
    grad_att = (grad_gated * gate).astype(BF16)
    g_exp[...] = jnp.where(head_mask(flat), expand(grad_att), 0.0).astype(BF16)
    grad_query = []
    grad_w_bias = jnp.zeros((heads, bias_norm_ref.shape[1]), F32)
    for b in range(num_cplx):
        keys = kv[b * tok:(b + 1) * tok, :chan]
        vals = kv[b * tok:(b + 1) * tok, chan:]
        p_wide = prob[b * per:(b + 1) * per, :]
        g_rows = g_exp[b * per:(b + 1) * per, :]
        grad_prob = mm_nt(g_rows, vals)
        grad_logits = (p_wide * (grad_prob - jnp.sum(p_wide * grad_prob, axis=-1, keepdims=True))).astype(BF16)
        gl_ref[b * per:(b + 1) * per, :] = grad_logits
        gl_wide = jnp.concatenate([grad_logits[i * heads:(i + 1) * heads, :] for i in range(row_count)], axis=1)
        grad_w_bias = grad_w_bias + mm(gl_wide, bias_norm_ref[b * row_count * tok:(b + 1) * row_count * tok, :])
        grad_query.append(fold(mm(grad_logits, keys)) * scale)
        gkv[b * tok:(b + 1) * tok, :chan] = (mm_tn(grad_logits, q_exp[b * per:(b + 1) * per, :]) * scale).astype(BF16)
        gkv[b * tok:(b + 1) * tok, chan:] = mm_tn(p_wide.astype(BF16), g_rows).astype(BF16)
    grad_query = jnp.concatenate(grad_query, axis=0)
    grad_query_bf = grad_query.astype(BF16)
    at = put(attn_ref, 0, mm_tn(act, grad_query_bf))
    at = put(attn_ref, at, mm_tn(a_all, gkv[...]))
    at = put(attn_ref, at, mm_tn(act, grad_gate))
    at = put(attn_ref, at, mm_tn(gated, grad_mid_bf))
    at = put(attn_ref, at, grad_w_bias)
    grad_q_bias = jnp.sum(grad_query, axis=0, keepdims=True)
    line = lax.broadcasted_iota(jnp.int32, (heads, LANES), 0)
    lines = jnp.zeros((heads, LANES), F32)
    for j in range(chan // LANES):
        lines = jnp.where(line == j, grad_q_bias[:, j * LANES:(j + 1) * LANES], lines)
    at = put(attn_ref, at, lines)
    attn_ref[at:, :] = jnp.zeros((attn_ref.shape[0] - at, LANES), BF16)
    part = mm_nt(gkv[...], w_kv_ref[...])
    for b in range(num_cplx):
        stage[:, b * row_count:(b + 1) * row_count, :] = part[b * tok:(b + 1) * tok, :].reshape(tok // row_count, row_count, chan)
    part_ref[...] = stage[...].astype(BF16)
    gact_ref[...] = mm_nt(grad_query_bf, w_q_ref[...]) + mm_nt(grad_gate, w_g_ref[...])


def single_track(tok, s_all, s_rows, ds_rows, mask, bias, bias_norm, weights):
    rows, chan = s_rows.shape
    flat = bias.shape[0]
    all_rows = PLANE * rows
    shapes = [((flat, tok), BF16), (s_all.shape, BF16), ((rows, chan), F32), ((rows, chan), F32), ((SHARDS * PIECE_ROWS[0], LANES), BF16), ((SHARDS * PIECE_ROWS[1], LANES), BF16)]
    return pl.pallas_call(
        functools.partial(single_kernel, tok),
        out_shape=[jax.ShapeDtypeStruct(*s) for s in shapes],
        in_specs=[pl.BlockSpec(memory_space=pltpu.VMEM)] * (6 + len(weights)),
        out_specs=[pl.BlockSpec(memory_space=pltpu.VMEM)] * len(shapes),
        scratch_shapes=[pltpu.VMEM((flat, chan), BF16), pltpu.VMEM((flat, chan), BF16), pltpu.VMEM((flat, tok), F32), pltpu.VMEM((all_rows, 2 * chan), BF16), pltpu.VMEM(s_all.shape, F32)],
        name="single_track",
        cost_estimate=pl.CostEstimate(flops=3 * 10**9, bytes_accessed=20 * 2**20, transcendentals=0),
    )(s_all, s_rows, ds_rows, mask, bias, bias_norm, *weights)


class Piece:
    def __init__(self, here, rows, whole, got, half, got_one, quarter, got_two, cross, total, send_sem, recv_sem):
        self.here, self.rows = here, rows
        self.whole, self.got, self.half = whole, got, half
        self.got_one, self.quarter, self.got_two = got_one, quarter, got_two
        self.cross, self.total = cross, total
        self.send_sem, self.recv_sem = send_sem, recv_sem

    def cut(self, ref, index, count=1):
        start = index * self.rows
        if not isinstance(start, int):
            start = pl.multiple_of(start, 16)
        return ref.at[pl.ds(start, count * self.rows)]

    def mine(self, route):
        return self.here['core'] * (SHARDS // 2) + route * PLANE

    def fan_out(self, phase, route, axis, src, dst):
        for k in range(1, SIDE):
            send(src(k), dst(k), self.send_sem.at[phase], self.recv_sem.at[phase, route], neighbour(self.here, axis, k))

    def swap_in(self, route):
        other = (1 - self.here['core']) * (SHARDS // 2) + route * PLANE
        send(self.cut(self.whole, other, PLANE), self.cut(self.got, route * PLANE, PLANE), self.send_sem.at[0], self.recv_sem.at[0, route], partner(self.here))

    def scatter_one(self, route):
        axis = ROUTES[route][0]
        spot = route * PLANE
        got = self.cut(self.got, spot, PLANE)
        wait_bytes(got, self.recv_sem.at[0, route])
        own = self.cut(self.whole, self.mine(route), PLANE)
        self.cut(self.half, spot, PLANE)[...] = (own[...].astype(F32) + got[...].astype(F32)).astype(BF16)
        self.fan_out(1, route, axis,
                     lambda k: self.cut(self.half, spot + (self.here[axis] + k) % SIDE * SIDE, SIDE),
                     lambda k: self.cut(self.got_one, (route * 3 + k - 1) * SIDE, SIDE))

    def scatter_two(self, route):
        first, axis = ROUTES[route][0], ROUTES[route][1]
        wait_bytes(self.cut(self.got_one, route * 3 * SIDE, 3 * SIDE), self.recv_sem.at[1, route])
        total = self.cut(self.half, route * PLANE + self.here[first] * SIDE, SIDE)[...].astype(F32)
        for k in range(3):
            total = total + self.cut(self.got_one, (route * 3 + k) * SIDE, SIDE)[...].astype(F32)
        self.cut(self.quarter, route * SIDE, SIDE)[...] = total.astype(BF16)
        self.fan_out(2, route, axis,
                     lambda k: self.cut(self.quarter, route * SIDE + (self.here[axis] + k) % SIDE),
                     lambda k: self.cut(self.got_two, route * 3 + k - 1))

    def exchange(self, route):
        second, axis = ROUTES[route][1], ROUTES[route][2]
        wait_bytes(self.cut(self.got_two, route * 3, 3), self.recv_sem.at[2, route])
        total = self.cut(self.quarter, route * SIDE + self.here[second])[...].astype(F32)
        for k in range(3):
            total = total + self.cut(self.got_two, route * 3 + k)[...].astype(F32)
        slot = self.cut(self.cross, route * SIDE + self.here[axis])
        slot[...] = total.astype(BF16)
        self.fan_out(3, route, axis, lambda k: slot, lambda k: slot)

    def gather_two(self, route):
        first, axis = ROUTES[route][0], ROUTES[route][1]
        wait_bytes(self.cut(self.got_two, route * 3, 3), self.recv_sem.at[3, route])
        total = self.cut(self.cross, route * SIDE)[...].astype(F32)
        for k in range(1, SIDE):
            total = total + self.cut(self.cross, route * SIDE + k)[...].astype(F32)
        shard = self.cut(self.total, self.mine(route) + self.here[first] * SIDE + self.here[axis])
        shard[...] = total.astype(BF16)
        self.fan_out(4, route, axis, lambda k: shard, lambda k: shard)

    def gather_one(self, route):
        axis = ROUTES[route][0]
        wait_bytes(self.cut(self.got_two, route * 3, 3), self.recv_sem.at[4, route])
        group = self.cut(self.total, self.mine(route) + self.here[axis] * SIDE, SIDE)
        self.fan_out(5, route, axis, lambda k: group, lambda k: group)

    def swap_out(self, route):
        wait_bytes(self.cut(self.got_one, route * 3 * SIDE, 3 * SIDE), self.recv_sem.at[5, route])
        own = self.cut(self.total, self.mine(route), PLANE)
        send(own, own, self.send_sem.at[6], self.recv_sem.at[6, route], partner(self.here))

    def finish(self, route):
        wait_bytes(self.cut(self.got, route * PLANE, PLANE), self.recv_sem.at[6, route])

    def drain(self):
        for phase, like in enumerate((self.got, self.got_one, self.got_two, self.got_two, self.got_two, self.got_one, self.got)):
            wait_bytes(like, self.send_sem.at[phase])

    STAGES = ('swap_in', 'scatter_one', 'scatter_two', 'exchange', 'gather_two', 'gather_one', 'swap_out', 'finish')

    def stage(self, number):
        for route in range(3):
            getattr(self, self.STAGES[number])(route)


def piece_scratch(rows):
    buffer = lambda shards: pltpu.VMEM((shards * rows, LANES), BF16)
    return [buffer(48), buffer(48), buffer(36), buffer(12), buffer(9), buffer(12), pltpu.SemaphoreType.DMA((7,)), pltpu.SemaphoreType.DMA((7, 3))]


def reduce_kernel(*refs):
    here = position()
    wholes, part_ref, outs, sum_ref = refs[:3], refs[3], refs[4:7], refs[7]
    part_got, part_send, part_recv, out_sem = refs[8:12]
    totals = refs[12:15]
    pieces = []
    for n in range(3):
        scratch = refs[15 + 8 * n:23 + 8 * n]
        pieces.append(Piece(here, PIECE_ROWS[n], wholes[n], *scratch[:6], totals[n], *scratch[6:]))
    meet([neighbour(here, 'x', k) for k in range(1, SIDE)] + [plane_member(here, k) for k in range(1, PLANE)] + [partner(here)])
    for piece in pieces:
        piece.stage(0)
    for piece in pieces:
        piece.stage(1)
    for k in range(1, PLANE):
        send(part_ref.at[(here['dap'] + k) % PLANE], part_got.at[k - 1], part_send, part_recv, plane_member(here, k))
    for number in range(2, 8):
        for piece in pieces:
            piece.stage(number)
    wait_bytes(part_got, part_recv)
    total = part_ref[here['dap']].astype(F32)
    for k in range(PLANE - 1):
        total = total + part_got[k].astype(F32)
    sum_ref[...] = total
    wait_bytes(part_got, part_send)
    copies = [pltpu.make_async_copy(totals[n], outs[n], out_sem.at[n]) for n in range(3)]
    for copy in copies:
        copy.start()
    for piece in pieces:
        piece.drain()
    for copy in copies:
        copy.wait()


def reduce_all(wholes, part):
    vmem = pl.BlockSpec(memory_space=pltpu.VMEM)
    shapes = [jax.ShapeDtypeStruct(w.shape, BF16) for w in wholes] + [jax.ShapeDtypeStruct(part.shape[1:], F32)]
    scratch = [pltpu.VMEM((PLANE - 1,) + part.shape[1:], BF16), pltpu.SemaphoreType.DMA, pltpu.SemaphoreType.DMA, pltpu.SemaphoreType.DMA((3,))]
    scratch = scratch + [pltpu.VMEM(w.shape, BF16) for w in wholes]
    for rows in PIECE_ROWS:
        scratch = scratch + piece_scratch(rows)
    return pl.pallas_call(
        reduce_kernel,
        out_shape=shapes,
        in_specs=[vmem] * 4,
        out_specs=[pl.BlockSpec(memory_space=pl.ANY)] * 3 + [vmem],
        scratch_shapes=scratch,
        compiler_params=pltpu.CompilerParams(collective_id=1, has_side_effects=True),
        name="reduce_all",
        cost_estimate=pl.CostEstimate(flops=10**9, bytes_accessed=20 * 2**20, transcendentals=0),
    )(*wholes, part)


LAYOUT = (('w_sa', 0, 0, 384, 1536), ('w_sb', 0, 4608, 384, 1536), ('w_so', 0, 9216, 1536, 384),
          ('w_q', 1, 0, 384, 384), ('w_kv', 1, 1152, 384, 768), ('w_g', 1, 3456, 384, 384), ('w_o', 1, 4608, 384, 384),
          ('w_pa', 2, 0, 128, 512), ('w_pb', 2, 512, 128, 512), ('w_po_t', 2, 1024, 128, 512))


def unpack_kernel(*refs):
    totals, outs, stages, sems = refs[:3], refs[3:15], refs[15:27], refs[27]
    copies = []
    for n, (name, piece, offset, rows, cols) in enumerate(LAYOUT):
        blocks = [totals[piece][offset + j * rows:offset + (j + 1) * rows, :].astype(F32) for j in range(cols // LANES)]
        if name == 'w_po_t':
            for j, block in enumerate(blocks):
                stages[n][j * LANES:(j + 1) * LANES, :] = block.T
        else:
            for j, block in enumerate(blocks):
                stages[n][:, j * LANES:(j + 1) * LANES] = block
        copies.append(pltpu.make_async_copy(stages[n], outs[n], sems.at[n]))
        copies[-1].start()
    stages[10][...] = totals[1][5760:5776, :].astype(F32)
    lines = totals[1][5776:5792, :].astype(F32)
    for j in range(3):
        stages[11][:, j * LANES:(j + 1) * LANES] = lines[j:j + 1, :]
    for n in (10, 11):
        copies.append(pltpu.make_async_copy(stages[n], outs[n], sems.at[n]))
        copies[-1].start()
    for copy in copies:
        copy.wait()


def unpack(totals):
    shapes = [(cols, rows) if name == 'w_po_t' else (rows, cols) for name, _, _, rows, cols in LAYOUT] + [(16, 128), (1, 384)]
    outs = pl.pallas_call(
        unpack_kernel,
        out_shape=[jax.ShapeDtypeStruct(shape, F32) for shape in shapes],
        in_specs=[pl.BlockSpec(memory_space=pltpu.VMEM)] * 3,
        out_specs=[pl.BlockSpec(memory_space=pl.ANY)] * 12,
        scratch_shapes=[pltpu.VMEM(shape, F32) for shape in shapes] + [pltpu.SemaphoreType.DMA((12,))],
        name="unpack",
        cost_estimate=pl.CostEstimate(flops=10**7, bytes_accessed=16 * 2**20, transcendentals=0),
    )(*totals)
    names = [entry[0] for entry in LAYOUT] + ['w_bias_t', 'q_bias']
    return dict(zip(names, outs))


def solution(mesh):
    pair_spec = P('dp', 'dap', None, None)
    single_spec = P('dp', 'dap', None)

    def body(pair_z, single_s, token_mask, dz_out, ds_out, w_pa, w_pb, w_po, w_bias, w_q, q_bias, w_kv, w_g, w_o, w_sa, w_sb, w_so):
        num_cplx, num_rows, tok, pair_dim = pair_z.shape
        chan = single_s.shape[-1]
        width = w_pa.shape[1]
        w_ab = jnp.concatenate([w_pa, w_pb], axis=1)
        w_ab_t = w_ab.T
        w_bias_t = w_bias.T
        z_rows = pair_z.reshape(-1, pair_dim)
        dz_rows = dz_out.reshape(-1, pair_dim)
        s_rows = single_s.reshape(-1, chan)
        z_new, bias, bias_norm, s_all = pair_forward(z_rows, w_ab, w_po, w_bias_t, s_rows, tok)
        grad_logits, part, gact, gmid, wide, attn = single_track(tok, s_all, s_rows, ds_out.reshape(-1, chan), token_mask, bias, bias_norm, (w_q, q_bias[None], w_kv, w_g, w_o, w_sa, w_sb, w_so))
        dz_in, dwab, dwpo_t = pair_backward(z_rows, z_new, dz_rows, grad_logits, w_ab, w_ab_t, w_po.T, w_bias_t, tok)
        pair = jnp.concatenate([dwab.reshape(pair_dim, -1, LANES), dwpo_t.reshape(pair_dim, -1, LANES)], axis=1).transpose(1, 0, 2).reshape(-1, LANES).astype(BF16)
        *totals, part_sum = reduce_all((wide, attn, pair), part)
        s_norm, s_inv = layer_norm(s_rows)
        ds_in = (gmid + norm_grad(s_norm, s_inv, gact + part_sum)).astype(BF16)
        grads = unpack(totals)
        ordered = (grads['w_pa'], grads['w_pb'], grads['w_po_t'], grads['w_bias_t'].T, grads['w_q'], grads['q_bias'][0], grads['w_kv'], grads['w_g'], grads['w_o'], grads['w_sa'], grads['w_sb'], grads['w_so'])
        return (dz_in.reshape(pair_z.shape), ds_in.reshape(single_s.shape)) + ordered

    in_specs = (pair_spec, single_spec, P('dp', None), pair_spec, single_spec) + (P(),) * 12
    out_specs = (pair_spec, single_spec) + (P(),) * 12
    return jax.shard_map(body, mesh=mesh, in_specs=in_specs, out_specs=out_specs, check_vma=False)
```
